32 devices in a mesh: grp: 8 (over y, x, core), blk: 4 (over z).
Axes of the slice: x: 2, y: 2, z: 4, core: 2. Of those that a mesh axis runs over, the one named last changes fastest.
Arguments:
- tokens: bfloat16 [256, 6144], P(('grp', 'blk')), may hold values from -6 to 6
- norm_gain: bfloat16 [6144], replicated, may hold values from 0.099609375 to 1.8984375
- expert_ids: int32 [256, 2], P(('grp', 'blk')), may hold values from 0 to 7, all different within a row; in each aligned block of 8 rows (0 to 7, 8 to 15, ...) at most 3 rows name the same one
- combine: float32 [256, 2], P(('grp', 'blk')), may hold values from 0.2 to 1
- w_gate: bfloat16 [6144, 65536], P(None, ('grp', 'blk')), may hold values from -0.078125 to 0.078125
- w_up: bfloat16 [6144, 65536], P(None, ('grp', 'blk')), may hold values from -0.078125 to 0.078125
- w_down: bfloat16 [65536, 6144], P(('grp', 'blk')), may hold values from -0.0625 to 0.0625
Outputs:
- layer_out: bfloat16 [256, 6144], P(('grp', 'blk'))
The draws below stay inside these ranges and needn't reach their ends.
Inputs may be any that keep to these rules, and one draw needn't show every extreme that they name: `expert_ids`: each row names 2 different experts; in the rows of one device no expert is named more than 3 times, a bound that some block reaches.
All inputs are finite; a program needn't handle non-finite values.
Results may differ from the reference program's by a relative error of at most 0.0075.
Values may be sent and summed in bfloat16 or wider, within the bound.
A program may use at most 128 MiB of HBM per device.

```python
import math
import jax
import jax.numpy as jnp
import numpy as np
from jax import lax

D = 6144
FF = 8192
E = 8
TOP = 2
TOK_DEV = 8
CAP = 3
TOKENS = 256
N_GRP = 8
N_BLK = 4


def steps_of(stream_key, shape, shards, smallest, largest):
    def one(axis_at, shards_of):
        steps = jax.random.uniform(jax.random.fold_in(jax.random.fold_in(stream_key, 6), axis_at), (shards_of,), jnp.float32, smallest / len(shards), largest / len(shards))
        return jnp.repeat(jnp.exp(steps), shape[axis_at] // shards_of).reshape((-1,) + (1,) * (len(shape) - axis_at - 1))

    loudness = one(*shards[0])
    for cut in shards[1:]:
        loudness = loudness * one(*cut)
    return loudness


def routed_block(rng, own, number, rows, number_of, top, reach, skew):
    ranking = jax.random.permutation(rng, number_of)
    packed, usual = shares(number_of, rows * top, reach, skew, True), shares(number_of, rows * top, reach, skew, False)
    places = jnp.arange(number_of)

    def named(lengths, turn):
        used = int((lengths > 0).sum())
        fixed = max(1, used // 4)
        passed = fixed + (places - fixed + turn * (used - fixed)) % max(1, number_of - fixed)
        return jnp.zeros((number_of,), jnp.int32).at[ranking[jnp.where(places < fixed, places, passed)]].set(jnp.asarray(lengths, jnp.int32))

    lengths = jnp.where(number % 4 == 0, named(packed, number // 4), named(usual, number - number // 4 - 1))
    mixed = jax.random.permutation(jax.random.fold_in(own, 3), number_of)
    source_of, receiver = mixed[0:number_of // 2 * 2:2], mixed[1:number_of // 2 * 2:2]
    margin = jnp.minimum(lengths[source_of] - 1, reach - lengths[receiver]) // 2
    margin = jnp.where((source_of == ranking[0]) | (receiver == ranking[0]) | (lengths[receiver] == 0), 0, jnp.maximum(margin, 0))
    passed = jax.random.randint(jax.random.fold_in(own, 4), (number_of // 2,), 0, 1 << 20) % (margin + 1)
    lengths = lengths.at[source_of].add(-passed).at[receiver].add(passed)
    items = jnp.searchsorted(jnp.cumsum(lengths), jnp.arange(rows * top), side="right").astype(jnp.int32)
    listing = items.reshape(top, rows).T
    listing = listing[jax.random.permutation(jax.random.fold_in(own, 1), rows)]
    turn = jax.random.randint(jax.random.fold_in(own, 2), (rows, 1), 0, top)
    return jnp.take_along_axis(listing, (jnp.arange(top)[None, :] + turn) % top, axis=1)


def shares(amount, total, reach, lean, full):
    portions = [(1 << 20) // math.isqrt(rank ** lean) + 1 for rank in range(1, amount + 1)]
    largest = reach if full else min(reach, max(-(-total // amount), total * portions[0] // sum(portions)))
    least = 1 if total - largest >= amount - 1 else 0
    counts, rest = [largest] + [least] * (amount - 1), total - largest - least * (amount - 1)
    while rest > 0:
        candidates = [i for i in range(1, amount) if counts[i] < largest] or [i for i in range(1, amount) if counts[i] < reach]
        whole, left = sum([portions[i] for i in candidates]), rest
        for i in candidates:
            extra = min(reach - counts[i], max(1, left * portions[i] // whole), rest)
            counts[i] = counts[i] + extra
            rest = rest - extra
    return np.array(counts)


def gaussian(rng, shape, width, bound, split=(), kind=jnp.bfloat16):
    factor_of = steps_of(rng, shape, split, -0.22, 0.18) if split else 1.0
    entries = jax.random.normal(rng, shape, jnp.float32) * width * factor_of
    return jnp.minimum(jnp.maximum(entries, -bound), bound).astype(kind)


def setup_inputs(seed: int = 0) -> dict:
    keys = jax.random.split(jax.random.key(seed), 8)
    tokens = gaussian(keys[0], (TOKENS, D), 1.0, 6.0, ((0, 32),))
    norm_gain = jnp.clip(1.0 + 0.18 * jax.random.normal(keys[1], (D,), jnp.float32), 0.099609375, 1.8984375).astype(jnp.bfloat16)
    expert_ids_keys = jax.random.split(jax.random.fold_in(keys[2], 1), TOKENS // TOK_DEV)
    expert_ids_turns = jax.random.permutation(jax.random.fold_in(keys[2], 3), TOKENS // TOK_DEV)
    expert_ids = jax.vmap(lambda own, number: routed_block(jax.random.fold_in(keys[2], 2), own, number, TOK_DEV, E, TOP, CAP, 2))(expert_ids_keys, expert_ids_turns).reshape((TOKENS, TOP))
    combine = jnp.clip(jnp.exp(math.log(1.0) - 1.609438 * jax.random.uniform(keys[3], (TOKENS, TOP), jnp.float32) ** steps_of(keys[3], (TOKENS, TOP), ((0, 32),), -0.2, 0.2)), 0.2, 1.0)
    w_gate = gaussian(keys[4], (D, E * FF), D ** -0.5, 0.078125, ((1, 32),))
    w_up = gaussian(keys[5], (D, E * FF), D ** -0.5, 0.078125, ((1, 32),))
    w_down = gaussian(keys[6], (E * FF, D), FF ** -0.5, 0.0625, ((0, 32),))
    return {"tokens": tokens, "norm_gain": norm_gain, "expert_ids": expert_ids, "combine": combine, "w_gate": w_gate, "w_up": w_up, "w_down": w_down}


epsilon = 1e-05

def reference(tokens, norm_gain, expert_ids, combine, w_gate, w_up, w_down):
    blocks = TOKENS // TOK_DEV
    pair_count = TOKENS * TOP
    per_block = TOK_DEV * TOP
    wide_tokens = tokens.astype(jnp.float32)
    scale_rows = lax.rsqrt(lax.optimization_barrier(jnp.mean(wide_tokens * wide_tokens, axis=1, keepdims=True)) + epsilon)
    normed = (wide_tokens * scale_rows * norm_gain.astype(jnp.float32)[None, :]).astype(jnp.bfloat16)
    pair_rows = jnp.repeat(normed, TOP, axis=0)
    block_ids = expert_ids.reshape(blocks, per_block)
    one_hot = (block_ids[:, :, None] == jnp.arange(E, dtype=jnp.int32)[None, None, :]).astype(jnp.int32)
    earlier = jnp.cumsum(one_hot, axis=1) - one_hot
    slot_index = lax.optimization_barrier(jnp.sum(earlier * one_hot, axis=2))
    global_slot = (slot_index + CAP * jnp.arange(blocks, dtype=jnp.int32)[:, None]).reshape(pair_count).astype(jnp.int32)
    route_ids = expert_ids.reshape(pair_count).astype(jnp.int32)
    slot_table = jnp.zeros((E, blocks * CAP), jnp.int32).at[route_ids, global_slot].set(jnp.arange(pair_count, dtype=jnp.int32))
    unit_count = E * FF // (N_GRP * N_BLK)

    def one_expert(expert_index):
        chosen = pair_rows[slot_table[expert_index]]
        gate_cols = lax.dynamic_slice_in_dim(w_gate, expert_index * FF, FF, 1)
        up_cols = lax.dynamic_slice_in_dim(w_up, expert_index * FF, FF, 1)
        down_rows = lax.dynamic_slice_in_dim(w_down, expert_index * FF, FF, 0)
        gate_val = jnp.dot(chosen, gate_cols, preferred_element_type=jnp.float32)
        up_val = jnp.dot(chosen, up_cols, preferred_element_type=jnp.float32)
        hidden = (jax.nn.silu(gate_val) * up_val).astype(jnp.bfloat16)

        def add_block(block_index, running):
            start = (block_index * unit_count).astype(jnp.int32)
            partial_value = jnp.dot(lax.dynamic_slice_in_dim(hidden, start, unit_count, 1), lax.dynamic_slice_in_dim(down_rows, start, unit_count, 0), preferred_element_type=jnp.float32)
            rounded = lax.optimization_barrier(partial_value.astype(jnp.bfloat16))
            return running + rounded.astype(jnp.float32)
        return lax.fori_loop(0, FF // unit_count, add_block, jnp.zeros((blocks * CAP, D), jnp.float32))
    outputs = lax.map(one_expert, jnp.arange(E, dtype=jnp.int32))
    pair_out = outputs[route_ids, global_slot]
    expert_mix = lax.optimization_barrier(jnp.sum(pair_out.reshape(TOKENS, TOP, D) * combine[:, :, None], axis=1))
    return (wide_tokens + expert_mix).astype(jnp.bfloat16)
```

```python
import functools
import numpy as np
import jax
import jax.numpy as jnp
from jax import lax
from jax.experimental import pallas as pl
from jax.experimental.pallas import tpu as pltpu
from jax.sharding import PartitionSpec as P

E = 8
TOP = 2
CAP = 3


epsilon = 1e-05
VMEM_LIMIT = 67_000_000
BF16, F32 = jnp.bfloat16, jnp.float32


def xor_index(index, offset, count):
    total, bit = 0, 1
    while bit < count:
        digit = (index // bit) % 2
        total = total + bit * ((1 - digit) if offset & bit else digit)
        bit *= 2
    return total


def tables(groups, blocks, splits, pair):
    lane = np.arange(groups * splits * CAP)
    send = [lane // (splits * CAP), (lane // CAP) % splits, lane % CAP]
    lane = np.arange(groups * pair * blocks * CAP)
    back = [lane // (pair * blocks * CAP), (lane // (blocks * CAP)) % pair, (lane // CAP) % blocks, lane % CAP]
    sources = 2 * groups
    gather = np.zeros((sources * splits * CAP,) * 2, np.float32)
    for q in range(splits):
        for s in range(sources):
            for c in range(CAP):
                gather[(q * sources + s) * CAP + c, (s * splits + q) * CAP + c] = 1
    rows = pair * blocks * groups * CAP
    spread = np.zeros((rows, rows), np.float32)
    for k in range(groups):
        for v in range(pair):
            for d in range(blocks):
                for c in range(CAP):
                    spread[((k * pair + v) * blocks + d) * CAP + c, ((v * blocks + d) * groups + k) * CAP + c] = 1
    return np.array(send, np.int32), np.array(back, np.int32), gather, spread


def layer_kernel(cfg, tok_ref, gain_ref, ids_ref, comb_ref, send_tab, back_tab, gather_ref, spread_ref,
                 wg_ref, wu_ref, wd_ref, out_ref,
                 gbuf, ubuf, dbuf, meta, toks, sbuf, rbuf, xbuf, gacc, uacc, hid, obuf, pbuf, qbuf, ybuf, vbuf,
                 wsem, msem, mrsem, tsem, trsem, ssem, srsem, psem, prsem, ysem, yrsem):
    groups, blocks, splits, pair, gslots, dslots = cfg
    me, depth = lax.axis_index("grp"), lax.axis_index("blk")
    tok_count, width = tok_ref.shape
    part = width // splits
    units = wg_ref.shape[1]
    unit_rows = splits * CAP
    back_rows = pair * blocks * CAP
    rows = blocks * groups * CAP

    def weights(kind, q):
        if kind == 0:
            return pltpu.make_async_copy(wg_ref.at[pl.ds(q * part, part)], gbuf.at[q % gslots], wsem.at[0, q])
        if kind == 1:
            return pltpu.make_async_copy(wu_ref.at[pl.ds(q * part, part)], ubuf.at[q % gslots], wsem.at[1, q])
        return pltpu.make_async_copy(wd_ref.at[:, pl.ds(q * part, part)], dbuf.at[q % dslots], wsem.at[2, q])

    for q in range(gslots):
        weights(0, q).start()
        weights(1, q).start()
    for q in range(dslots):
        weights(2, q).start()

    group_of = [{"grp": xor_index(me, k, groups), "blk": depth} for k in range(groups)]
    block_of = [{"grp": me, "blk": xor_index(depth, d, blocks)} for d in range(blocks)]
    barrier = pltpu.get_barrier_semaphore()
    for peer in group_of[1:] + block_of[1:]:
        pl.semaphore_signal(barrier, inc=1, device_id=peer, device_id_type=pl.DeviceIdType.MESH)

    lane = lax.broadcasted_iota(jnp.int32, (tok_count, 128), 1)
    ids = ids_ref[...].astype(F32)
    comb = comb_ref[...]
    meta[0] = jnp.where(lane == 0, ids[:, 0:1], jnp.where(lane == 1, ids[:, 1:2],
                        jnp.where(lane == 2, comb[:, 0:1], jnp.where(lane == 3, comb[:, 1:2], 0.0))))
    wide = tok_ref[...].astype(F32)
    scale = lax.rsqrt(jnp.mean(wide * wide, axis=1, keepdims=True) + epsilon)
    normed = wide * scale * gain_ref[...].astype(F32)
    toks[0] = jnp.concatenate([normed[:, q * part:(q + 1) * part] for q in range(splits)], axis=0).astype(BF16)
    pl.semaphore_wait(barrier, groups + blocks - 2)

    def remote(src, dst, send, recv, peer):
        return pltpu.make_async_remote_copy(src_ref=src, dst_ref=dst, send_sem=send, recv_sem=recv,
                                            device_id=peer, device_id_type=pl.DeviceIdType.MESH)

    meta_out = [None] + [remote(meta.at[0], meta.at[d], msem.at[d], mrsem.at[d], block_of[d]) for d in range(1, blocks)]
    toks_out = [None] + [remote(toks.at[0], toks.at[d], tsem.at[d], trsem.at[d], block_of[d]) for d in range(1, blocks)]
    for d in range(1, blocks):
        meta_out[d].start()
        toks_out[d].start()

    def matches(info, expert, slot):
        first = expert == info[:, 0:1]
        second = expert == info[:, 1:2]
        member = jnp.where(first, 1.0, jnp.where(second, 1.0, 0.0))
        row = lax.broadcasted_iota(jnp.int32, member.shape, 0)
        earlier = jnp.zeros_like(member)
        for t in range(tok_count - 1):
            earlier = earlier + jnp.where(row > t, member[t:t + 1, :], 0.0)
        at_slot = jnp.where(earlier == slot, 1.0, 0.0)
        return jnp.where(first, at_slot, 0.0), jnp.where(second, at_slot, 0.0)

    send_expert = (send_tab[0:1, :] ^ me).astype(F32)
    send_split, send_slot = send_tab[1:2, :], send_tab[2:3, :].astype(F32)
    back_expert = (back_tab[0:1, :] ^ me).astype(F32)
    back_pair, back_depth, back_slot = back_tab[1:2, :], back_tab[2:3, :], back_tab[3:4, :].astype(F32)

    slots_out = {}
    for d in range(blocks):
        if d:
            meta_out[d].wait_recv()
            toks_out[d].wait_recv()
        one, two = matches(meta[d], send_expert, send_slot)
        both = one + two
        placer = jnp.concatenate([jnp.where(send_split == q, both, 0.0) for q in range(splits)], axis=0).astype(BF16)
        placed = lax.dot_general(placer, toks[d], (((0,), (0,)), ((), ())), preferred_element_type=F32)
        for k in range(1, groups):
            sbuf[d, k] = placed[k * unit_rows:(k + 1) * unit_rows].astype(BF16)
        rbuf[d, 0] = placed[:unit_rows].astype(BF16)
        for k in range(groups - 1, 0, -1):
            slots_out[d, k] = remote(sbuf.at[d, k], rbuf.at[d, k], ssem.at[d, k], srsem.at[d, k], group_of[k])
            slots_out[d, k].start()

    mixes = []
    for d in range(blocks):
        one, two = matches(meta[d], back_expert, back_slot)
        mix = jnp.where(back_depth == d, one * meta[d][:, 2:3] + two * meta[d][:, 3:4], 0.0)
        mixes += [jnp.where(back_pair == v, mix, 0.0) for v in range(pair)]
    mix = jnp.concatenate(mixes, axis=0)
    mix_high = mix.astype(BF16)
    mix_low = (mix - mix_high.astype(F32)).astype(BF16)

    half = 2 * groups * CAP
    for h in range(blocks // 2):
        for d in (2 * h, 2 * h + 1):
            for k in range(1, groups):
                slots_out[d, k].wait_recv()
        held = jnp.concatenate([rbuf[d, k].astype(F32) for d in (2 * h, 2 * h + 1) for k in range(groups)], axis=0).astype(BF16)
        sorted_rows = jnp.dot(gather_ref[...], held, preferred_element_type=F32).astype(BF16)
        for q in range(splits):
            xbuf[q, h * half:(h + 1) * half, :] = sorted_rows[q * half:(q + 1) * half]

    tile = min(units, 512)
    gacc[...] = jnp.zeros_like(gacc)
    uacc[...] = jnp.zeros_like(uacc)
    for q in range(splits):
        weights(0, q).wait()
        weights(1, q).wait()

        @pl.loop(0, units // tile)
        def _(n):
            cols = pl.ds(pl.multiple_of(n * tile, tile), tile)
            gacc[:, cols] += jnp.dot(xbuf[q], gbuf[q % gslots, :, cols], preferred_element_type=F32)
            uacc[:, cols] += jnp.dot(xbuf[q], ubuf[q % gslots, :, cols], preferred_element_type=F32)

        if q + gslots < splits:
            weights(0, q + gslots).start()
            weights(1, q + gslots).start()

    @pl.loop(0, units // tile)
    def _(n):
        cols = pl.ds(pl.multiple_of(n * tile, tile), tile)
        gate = gacc[:, cols]
        hid[:, cols] = (gate / (1.0 + jnp.exp(-gate)) * uacc[:, cols]).astype(BF16)

    back_out = {}
    steps = splits // pair
    for j in range(steps):
        for v in range(pair):
            q = j * pair + v
            weights(2, q).wait()

            @pl.loop(0, part // 256)
            def _(n):
                cols = pl.ds(pl.multiple_of(n * 256, 256), 256)
                obuf[v * rows:(v + 1) * rows, cols] = jnp.dot(
                    hid[...], dbuf[q % dslots, :, cols], preferred_element_type=F32).astype(BF16)

            if q + dslots < splits:
                weights(2, q + dslots).start()
        spread = jnp.dot(spread_ref[...], obuf[...], preferred_element_type=F32)
        for k in range(1, groups):
            pbuf[j, k] = spread[k * back_rows:(k + 1) * back_rows].astype(BF16)
        qbuf[j, 0] = spread[:back_rows].astype(BF16)
        for k in range(groups - 1, 0, -1):
            back_out[j, k] = remote(pbuf.at[j, k], qbuf.at[j, k], psem.at[j, k], prsem.at[j, k], group_of[k])
            back_out[j, k].start()

    mixed_out, own = {}, []
    span = pair * tok_count
    for j in range(steps):
        for k in range(1, groups):
            back_out[j, k].wait_recv()
        held = jnp.concatenate([qbuf[j, k].astype(F32) for k in range(groups)], axis=0).astype(BF16)
        mixed = (jnp.dot(mix_high, held, preferred_element_type=F32)
                 + jnp.dot(mix_low, held, preferred_element_type=F32))
        own.append(mixed[:span])
        for d in range(1, blocks):
            ybuf[j, d] = mixed[d * span:(d + 1) * span].astype(BF16)
        for d in range(1, blocks):
            mixed_out[j, d] = remote(ybuf.at[j, d], vbuf.at[j, d], ysem.at[j, d], yrsem.at[j, d], block_of[d])
            mixed_out[j, d].start()

    for j in range(steps):
        total = own[j]
        for d in range(1, blocks):
            mixed_out[j, d].wait_recv()
            total = total + vbuf[j, d].astype(F32)
        for v in range(pair):
            cols = slice((j * pair + v) * part, (j * pair + v + 1) * part)
            out_ref[:, cols] = (tok_ref[:, cols].astype(F32) + total[v * tok_count:(v + 1) * tok_count]).astype(BF16)

    for copies in (meta_out[1:], toks_out[1:], slots_out.values(), back_out.values(), mixed_out.values()):
        for copy in copies:
            copy.wait_send()


def fused(groups, blocks, tokens, norm_gain, expert_ids, combine, w_gate, w_up, w_down):
    tok_count, width = tokens.shape
    units = w_gate.shape[1]
    splits, pair = 8, 2
    gslots, dslots = 6, 4
    part = width // splits
    rows = blocks * groups * CAP
    steps = splits // pair
    send, back, gather, spread = tables(groups, blocks, splits, pair)
    vmem = pl.BlockSpec(memory_space=pltpu.VMEM)
    dma = pltpu.SemaphoreType.DMA
    unit_rows, back_rows, span = splits * CAP, pair * blocks * CAP, pair * tok_count
    return pl.pallas_call(
        functools.partial(layer_kernel, (groups, blocks, splits, pair, gslots, dslots)),
        out_shape=jax.ShapeDtypeStruct((tok_count, width), BF16),
        in_specs=[vmem] * 8 + [pl.BlockSpec(memory_space=pl.ANY)] * 3,
        out_specs=vmem,
        scratch_shapes=[
            pltpu.VMEM((gslots, part, units), BF16),
            pltpu.VMEM((gslots, part, units), BF16),
            pltpu.VMEM((dslots, units, part), BF16),
            pltpu.VMEM((blocks, tok_count, 128), F32),
            pltpu.VMEM((blocks, splits * tok_count, part), BF16),
            pltpu.VMEM((blocks, groups, unit_rows, part), BF16),
            pltpu.VMEM((blocks, groups, unit_rows, part), BF16),
            pltpu.VMEM((splits, rows, part), BF16),
            pltpu.VMEM((rows, units), F32),
            pltpu.VMEM((rows, units), F32),
            pltpu.VMEM((rows, units), BF16),
            pltpu.VMEM((pair * rows, part), BF16),
            pltpu.VMEM((steps, groups, back_rows, part), BF16),
            pltpu.VMEM((steps, groups, back_rows, part), BF16),
            pltpu.VMEM((steps, blocks, span, part), BF16),
            pltpu.VMEM((steps, blocks, span, part), BF16),
            dma((3, splits)),
            dma((blocks,)), dma((blocks,)), dma((blocks,)), dma((blocks,)),
            dma((blocks, groups)), dma((blocks, groups)),
            dma((steps, groups)), dma((steps, groups)),
            dma((steps, blocks)), dma((steps, blocks)),
        ],
        compiler_params=pltpu.CompilerParams(collective_id=0, has_side_effects=True, vmem_limit_bytes=VMEM_LIMIT),
    )(tokens, norm_gain.reshape(1, width), expert_ids, combine, jnp.asarray(send), jnp.asarray(back),
      jnp.asarray(gather, BF16), jnp.asarray(spread, BF16), w_gate, w_up, w_down)


def on_device(tokens, norm_gain, expert_ids, combine, w_gate, w_up, w_down):
    group_count = lax.axis_size("grp")
    block_count = lax.axis_size("blk")
    per_group = group_count // E
    tok_count = tokens.shape[0]
    if group_count == E and block_count == 4 and tok_count == 8 and tokens.shape[1] % 2048 == 0:
        return fused(
            group_count, block_count, tokens, norm_gain, expert_ids, combine, w_gate, w_up, w_down
        )
    model_width = tokens.shape[1]
    wide_tokens = tokens.astype(jnp.float32)
    scale_rows = lax.rsqrt(jnp.mean(wide_tokens * wide_tokens, axis=1, keepdims=True) + epsilon)
    normed = (wide_tokens * scale_rows * norm_gain.astype(jnp.float32)[None, :]).astype(
        jnp.bfloat16
    )
    pair_rows = jnp.repeat(normed, TOP, axis=0)
    route_ids = expert_ids.reshape(tok_count * TOP)
    one_hot = (route_ids[:, None] == jnp.arange(E, dtype=jnp.int32)[None, :]).astype(jnp.int32)
    earlier = jnp.cumsum(one_hot, axis=0) - one_hot
    slot_index = jnp.sum(earlier * one_hot, axis=1)
    slot_match = (
        slot_index[None, None, :] == jnp.arange(CAP, dtype=jnp.int32)[None, :, None]
    ).astype(jnp.int32)
    placer = (one_hot.T[:, None, :] * slot_match).astype(jnp.bfloat16)
    buffer = jnp.einsum(
        "ecp,pd->ecd", placer, pair_rows, preferred_element_type=jnp.float32
    ).astype(jnp.bfloat16)
    outgoing = jnp.repeat(buffer, per_group, axis=0)
    arrived = lax.all_to_all(outgoing, "grp", split_axis=0, concat_axis=0, tiled=True)
    flat_rows = arrived.reshape(group_count * CAP, model_width)
    shard_rows = lax.all_gather(flat_rows, "blk", axis=0, tiled=True)
    gate_val = jnp.dot(shard_rows, w_gate, preferred_element_type=jnp.float32)
    up_val = jnp.dot(shard_rows, w_up, preferred_element_type=jnp.float32)
    hidden = (jax.nn.silu(gate_val) * up_val).astype(jnp.bfloat16)
    partial_value = jnp.dot(hidden, w_down, preferred_element_type=jnp.float32)
    rounded = lax.optimization_barrier(partial_value.astype(jnp.bfloat16))
    own_rows = lax.psum_scatter(
        rounded.astype(jnp.float32).astype(jnp.bfloat16), "blk", scatter_dimension=0, tiled=True
    ).astype(jnp.float32)
    home_terms = own_rows.reshape(group_count, CAP, model_width)
    returned = lax.all_to_all(
        home_terms.astype(jnp.bfloat16), "grp", split_axis=0, concat_axis=0, tiled=True
    ).astype(home_terms.dtype)
    expert_out = jnp.sum(returned.reshape(E, per_group, CAP, model_width), axis=1)
    pair_out = expert_out.reshape(E * CAP, model_width)[route_ids * CAP + slot_index]
    expert_mix = jnp.sum(
        pair_out.reshape(tok_count, TOP, model_width) * combine[:, :, None], axis=1
    )
    return (wide_tokens + expert_mix).astype(jnp.bfloat16)


def solution(mesh):
    return jax.shard_map(
        on_device,
        mesh=mesh,
        in_specs=(
            P(("grp", "blk"), None),
            P(),
            P(("grp", "blk"), None),
            P(("grp", "blk"), None),
            P(None, ("grp", "blk")),
            P(None, ("grp", "blk")),
            P(("grp", "blk"), None),
        ),
        out_specs=P(("grp", "blk"), None),
        check_vma=False,
    )
```
